32 devices in a mesh: south: 4 (over z), east: 4 (over y, x), down: 2 (over core).
Axes of the slice: x: 2, y: 2, z: 4, core: 2. Of those that a mesh axis runs over, the one named last changes fastest.
Arguments:
- initial_scalar_state: float32 [16, 128, 256, 128], P('south', 'east', 'down'), may hold values from 0.2 to 1.8
- scaled_wind_second: float32 [16, 128, 256, 128], P('south', 'east', 'down'), may hold values from -0.3 to 0.3
- scaled_wind_first: float32 [16, 128, 256, 128], P('south', 'east', 'down'), may hold values from -0.3 to 0.3
- scaled_wind_third: float32 [16, 128, 256, 128], P('south', 'east', 'down'), may hold values from -0.3 to 0.3
Outputs:
- temperature_end: float32 [16, 128, 256, 128], P('south', 'east', 'down')
The draws below stay inside these ranges and needn't reach their ends.
All inputs are finite; a program needn't handle non-finite values.
Results may differ from the reference program's by a relative error of at most 0.00002.
Values sent between devices are 32-bit elements; how exact they have to be, the bound alone decides.
No kernel may reach another device: no remote copies, remote signals or barrier semaphores. Data moves between devices by JAX's collectives and lax.ppermute only.
A program may use at most 448 MiB of HBM per device.

```python
import jax
import jax.numpy as jnp
from jax import lax

SECOND_AXIS_SIZE = 16
FIRST_AXIS_SIZE = 128
THIRD_AXIS_SIZE = 256
HEIGHT_COUNT = 128
STEPS = 4


def steps_of(stream_key, extent, split, low, largest):
    gain, own = 1.0, jax.random.fold_in(stream_key, 6)
    for axis_at, shards_of in split:
        steps = jnp.exp(jax.random.uniform(jax.random.fold_in(own, axis_at), (shards_of,), jnp.float32, low / len(split), largest / len(split)))
        gain = gain * jnp.repeat(steps, extent[axis_at] // shards_of).reshape([-1 if axis == axis_at else 1 for axis in range(len(extent))])
    return gain


def setup_inputs(seed: int = 0) -> dict:
    arg_keys = jax.random.split(jax.random.key(seed), 5)
    initial_scalar_state = jnp.clip(0.2 + 1.5999999 * jax.random.uniform(arg_keys[0], (SECOND_AXIS_SIZE, FIRST_AXIS_SIZE, THIRD_AXIS_SIZE, HEIGHT_COUNT), jnp.float32) ** steps_of(arg_keys[0], (SECOND_AXIS_SIZE, FIRST_AXIS_SIZE, THIRD_AXIS_SIZE, HEIGHT_COUNT), ((0, 4), (1, 4), (2, 2)), -0.2, 0.2), 0.2, 1.8)
    scaled_wind_second = jnp.clip(jax.random.uniform(arg_keys[1], (SECOND_AXIS_SIZE, FIRST_AXIS_SIZE, THIRD_AXIS_SIZE, HEIGHT_COUNT), jnp.float32, -0.3, 0.3) * steps_of(arg_keys[1], (SECOND_AXIS_SIZE, FIRST_AXIS_SIZE, THIRD_AXIS_SIZE, HEIGHT_COUNT), ((0, 4), (1, 4), (2, 2)), -0.4, 0.0), -0.3, 0.3)
    scaled_wind_first = jnp.clip(jax.random.uniform(arg_keys[2], (SECOND_AXIS_SIZE, FIRST_AXIS_SIZE, THIRD_AXIS_SIZE, HEIGHT_COUNT), jnp.float32, -0.3, 0.3) * steps_of(arg_keys[2], (SECOND_AXIS_SIZE, FIRST_AXIS_SIZE, THIRD_AXIS_SIZE, HEIGHT_COUNT), ((0, 4), (1, 4), (2, 2)), -0.4, 0.0), -0.3, 0.3)
    scaled_wind_third = jnp.clip(jax.random.uniform(arg_keys[3], (SECOND_AXIS_SIZE, FIRST_AXIS_SIZE, THIRD_AXIS_SIZE, HEIGHT_COUNT), jnp.float32, -0.3, 0.3) * steps_of(arg_keys[3], (SECOND_AXIS_SIZE, FIRST_AXIS_SIZE, THIRD_AXIS_SIZE, HEIGHT_COUNT), ((0, 4), (1, 4), (2, 2)), -0.4, 0.0), -0.3, 0.3)
    return {"initial_scalar_state": initial_scalar_state, "scaled_wind_second": scaled_wind_second, "scaled_wind_first": scaled_wind_first, "scaled_wind_third": scaled_wind_third}


def strip_edges(values, dims):
    for dim in dims:
        values = lax.slice_in_dim(values, 1, values.shape[dim] - 1, axis=dim)
    return values


def neighbour(values, dim, start, dims):
    others = [other for other in dims if other != dim]
    values = strip_edges(values, others)
    return lax.slice_in_dim(values, start, start + values.shape[dim] - 2, axis=dim)


def update_lone_timestep(padded_with_margin, scaled_wind_second, scaled_wind_first, scaled_wind_third):
    middle = strip_edges(padded_with_margin, (0, 1, 2))
    lower = [neighbour(padded_with_margin, dim, 0, (0, 1, 2)) for dim in (0, 1, 2)]
    upper = [neighbour(padded_with_margin, dim, 2, (0, 1, 2)) for dim in (0, 1, 2)]
    slopes = [above - below for above, below in zip(upper, lower)]
    smooth_rate = 0.05
    spread = lower[0] + upper[0] + lower[1] + upper[1] + lower[2] + upper[2] - 6.0 * middle
    return middle - scaled_wind_second * slopes[0] - scaled_wind_first * slopes[1] - scaled_wind_third * slopes[2] + smooth_rate * spread


def reference(initial_scalar_state, scaled_wind_second, scaled_wind_first, scaled_wind_third):
    for step in range(STEPS):
        initial_scalar_state = update_lone_timestep(jnp.pad(initial_scalar_state, ((1, 1), (1, 1), (1, 1), (0, 0)), mode="wrap"), scaled_wind_second, scaled_wind_first, scaled_wind_third)
    return initial_scalar_state
```

```python
import functools

import jax
import jax.numpy as jnp
from jax import lax
from jax.experimental import pallas as pl
from jax.experimental.pallas import tpu as pltpu
from jax.sharding import PartitionSpec as P

STEPS = 4
CHUNKS = 2
SMOOTH_RATE = 0.05


def shift(values, axis, step):
    size = lax.axis_size(axis)
    return lax.ppermute(values, axis, [(i, (i + step) % size) for i in range(size)])


def exchange(first, last, axis):
    if lax.axis_size(axis) == 2:
        other = shift(jnp.stack([last, first]), axis, 1)
        return other[0], other[1]
    return shift(last, axis, 1), shift(first, axis, -1)


def step_kernel(*refs, planes, rows, edges, aliased):
    (state, above_row, below_row, lead_row, trail_row, j_before, j_after,
     k_before, k_after, wind_j, wind_i, wind_k) = refs[:12]
    outs = refs[12 + aliased:]
    out = outs[0]
    at = pl.program_id(0)
    is_first, is_last = at == 0, at == pl.num_programs(0) - 1
    levels = lax.broadcasted_iota(jnp.int32, state.shape[2:], 0)
    k_size = state.shape[2]
    at_bottom, at_top = levels == 0, levels == k_size - 1
    for j in range(planes):
        for r in range(rows):
            row = at * rows + r
            here = state[j, r]
            i_low = state[j, r - 1] if r else jnp.where(is_first, lead_row[j, 0], above_row[j, 0])
            i_high = (
                state[j, r + 1] if r < rows - 1
                else jnp.where(is_last, trail_row[j, 0], below_row[j, 0])
            )
            j_low = state[j - 1, r] if j else j_before[r]
            j_high = state[j + 1, r] if j < planes - 1 else j_after[r]
            k_low = jnp.where(at_bottom, k_before[j, pl.ds(row, 1), :], pltpu.roll(here, 1, 0))
            k_high = jnp.where(
                at_top, k_after[j, pl.ds(row, 1), :], pltpu.roll(here, k_size - 1, 0)
            )
            spread = j_low + j_high + i_low + i_high + k_low + k_high - 6.0 * here
            new = (
                here
                - wind_j[j, r] * (j_high - j_low)
                - wind_i[j, r] * (i_high - i_low)
                - wind_k[j, r] * (k_high - k_low)
                + SMOOTH_RATE * spread
            )
            out[j, r] = new
            if edges:
                first_plane, last_plane, k_first, k_last = outs[1:]
                k_first[j, pl.ds(row, 1), :] = new[:1]
                k_last[j, pl.ds(row, 1), :] = new[k_size - 1:]
                if j == 0:
                    first_plane[r] = new
                if j == planes - 1:
                    last_plane[r] = new


def step_chunk(state, start, lead, trail, j_halo, k_halo, winds, chunk, length, edges, base):
    planes, full, k_size, heights = winds[0].shape
    rows = next(n for n in (4, 2, 1) if length % n == 0)
    steps = length // rows
    tail = (k_size, heights)

    def block(first):
        return pl.BlockSpec((planes, rows) + tail, lambda g: (0, first // rows + g, 0, 0))

    def one_row(row_of):
        return pl.BlockSpec((planes, 1) + tail, lambda g: (0, row_of(g), 0, 0))

    plane = pl.BlockSpec((rows,) + tail, lambda g: (g, 0, 0))
    line = pl.BlockSpec((planes, length, heights), lambda g: (0, 0, 0))
    in_specs = [
        block(start),
        one_row(lambda g: start + jnp.maximum(g * rows - 1, 0)),
        one_row(lambda g: start + jnp.minimum(g * rows + rows, length - 1)),
        one_row(lambda g: lead[1]),
        one_row(lambda g: trail[1]),
        plane, plane, line, line,
    ] + [block(chunk * length)] * 3
    operands = [state, state, state, lead[0], trail[0], *j_halo, *k_halo, *winds]
    aliases = {}
    dtype = state.dtype
    if edges:
        out_specs = [block(0), plane, plane, line, line]
        out_shape = [
            jax.ShapeDtypeStruct((planes, length) + tail, dtype),
            *[jax.ShapeDtypeStruct((length,) + tail, dtype)] * 2,
            *[jax.ShapeDtypeStruct((planes, length, heights), dtype)] * 2,
        ]
    else:
        out_specs = [block(chunk * length)]
        out_shape = [jax.ShapeDtypeStruct((planes, full) + tail, dtype)]
        if base is not None:
            aliases = {len(operands): 0}
            operands.append(base)
            in_specs.append(pl.BlockSpec(memory_space=pl.ANY))
    cells = planes * length * k_size * heights
    return pl.pallas_call(
        functools.partial(
            step_kernel, planes=planes, rows=rows, edges=edges, aliased=len(aliases)
        ),
        grid=(steps,),
        in_specs=in_specs,
        out_specs=out_specs,
        out_shape=out_shape,
        input_output_aliases=aliases,
        cost_estimate=pl.CostEstimate(flops=25 * cells, bytes_accessed=24 * cells, transcendentals=0),
        compiler_params=pltpu.CompilerParams(dimension_semantics=("arbitrary",)),
    )(*operands)


def on_device(initial_scalar_state, *winds):
    x = initial_scalar_state
    full = x.shape[1]
    chunks = CHUNKS if full % CHUNKS == 0 else 1
    length = full // chunks
    parts = [slice(c * length, (c + 1) * length) for c in range(chunks)]
    j_halos = [exchange(x[0, part], x[-1, part], "south") for part in parts]
    i_halo = exchange(x[:, :1], x[:, -1:], "east")
    k_halos = [exchange(x[:, part, 0], x[:, part, -1], "down") for part in parts]
    states = [(x, c * length) for c in range(chunks)]
    for step in range(STEPS):
        final = step == STEPS - 1
        base = None
        made = []
        for c in range(chunks):
            state, start = states[c]
            lead = (states[c - 1][0], states[c - 1][1] + length - 1) if c else (i_halo[0], 0)
            trail = states[c + 1] if c < chunks - 1 else (i_halo[1], 0)
            out = step_chunk(
                state, start, lead, trail, j_halos[c], k_halos[c], winds, c, length,
                not final, base,
            )
            if final:
                base = out[0]
                continue
            fresh, first_plane, last_plane, k_first, k_last = out
            made.append((fresh, 0))
            j_halos[c] = exchange(first_plane, last_plane, "south")
            k_halos[c] = exchange(k_first, k_last, "down")
        if final:
            return base
        states = made
        i_halo = exchange(made[0][0][:, :1], made[-1][0][:, -1:], "east")


def solution(mesh):
    placed = P("south", "east", "down", None)
    return jax.shard_map(
        on_device,
        mesh=mesh,
        in_specs=(placed,) * 4,
        out_specs=placed,
        check_vma=False,
    )
```

```python
import functools

import jax
import jax.numpy as jnp
from jax import lax
from jax.experimental import pallas as pl
from jax.experimental.pallas import tpu as pltpu
from jax.sharding import PartitionSpec as P


STEPS = 4
CHUNK_EIGHTHS = (3, 3, 2)
SMOOTH_RATE = 0.05


def shift(values, axis, step):
    size = lax.axis_size(axis)
    return lax.ppermute(values, axis, [(i, (i + step) % size) for i in range(size)])


def exchange(first, last, axis):
    if lax.axis_size(axis) == 2:
        other = shift(jnp.stack([last, first]), axis, 1)
        return other[0], other[1]
    return shift(last, axis, 1), shift(first, axis, -1)


def exchange_south(first, last):
    before = shift(last, "south", 1)
    after = shift(first, "south", -1)
    return before, after


def step_kernel(*refs, planes, rows, edges, aliased):
    (state, above_row, below_row, lead_row, trail_row, j_before, j_after,
     k_before, k_after, wind_j, wind_i, wind_k) = refs[:12]
    outs = refs[12 + aliased:]
    out = outs[0]
    at = pl.program_id(0)
    is_first, is_last = at == 0, at == pl.num_programs(0) - 1
    levels = lax.broadcasted_iota(jnp.int32, state.shape[2:], 0)
    k_size = state.shape[2]
    at_bottom, at_top = levels == 0, levels == k_size - 1
    for j in range(planes):
        for r in range(rows):
            row = at * rows + r
            here = state[j, r]
            i_low = state[j, r - 1] if r else jnp.where(is_first, lead_row[j, 0], above_row[j, 0])
            i_high = (
                state[j, r + 1] if r < rows - 1
                else jnp.where(is_last, trail_row[j, 0], below_row[j, 0])
            )
            j_low = state[j - 1, r] if j else j_before[r]
            j_high = state[j + 1, r] if j < planes - 1 else j_after[r]
            k_low = jnp.where(at_bottom, k_before[j, pl.ds(row, 1), :], pltpu.roll(here, 1, 0))
            k_high = jnp.where(
                at_top, k_after[j, pl.ds(row, 1), :], pltpu.roll(here, k_size - 1, 0)
            )
            spread = j_low + j_high + i_low + i_high + k_low + k_high - 6.0 * here
            new = (
                here
                - wind_j[j, r] * (j_high - j_low)
                - wind_i[j, r] * (i_high - i_low)
                - wind_k[j, r] * (k_high - k_low)
                + SMOOTH_RATE * spread
            )
            out[j, r] = new
            if edges:
                first_plane, last_plane, k_first, k_last = outs[1:]
                k_first[j, pl.ds(row, 1), :] = new[:1]
                k_last[j, pl.ds(row, 1), :] = new[k_size - 1:]
                if j == 0:
                    first_plane[r] = new
                if j == planes - 1:
                    last_plane[r] = new


def plane_kernel(*refs, rows, halo):
    (state, above_row, below_row, lead_row, trail_row, low, high,
     k_before, k_after, wind_j, wind_i, wind_k) = refs[:12]
    out = refs[-1]
    at = pl.program_id(1)
    is_first, is_last = at == 0, at == pl.num_programs(1) - 1
    is_start = pl.program_id(0) == 0
    levels = lax.broadcasted_iota(jnp.int32, state.shape[2:], 0)
    k_size = state.shape[2]
    at_bottom, at_top = levels == 0, levels == k_size - 1
    for r in range(rows):
        row = at * rows + r
        here = state[0, r]
        i_low = state[0, r - 1] if r else jnp.where(is_first, lead_row[0, 0], above_row[0, 0])
        i_high = (
            state[0, r + 1] if r < rows - 1
            else jnp.where(is_last, trail_row[0, 0], below_row[0, 0])
        )
        j_low, j_high = low[0, r], high[0, r]
        if halo:
            j_before, j_after = refs[12:14]
            j_low = jnp.where(is_start, j_before[r], j_low)
            j_high = jnp.where(is_start, j_high, j_after[r])
        k_low = jnp.where(at_bottom, k_before[0, pl.ds(row, 1), :], pltpu.roll(here, 1, 0))
        k_high = jnp.where(at_top, k_after[0, pl.ds(row, 1), :], pltpu.roll(here, k_size - 1, 0))
        spread = j_low + j_high + i_low + i_high + k_low + k_high - 6.0 * here
        out[0, r] = (
            here
            - wind_j[0, r] * (j_high - j_low)
            - wind_i[0, r] * (i_high - i_low)
            - wind_k[0, r] * (k_high - k_low)
            + SMOOTH_RATE * spread
        )


def rows_for(*sizes):
    return next(n for n in (4, 2, 1) if all(size % n == 0 for size in sizes))


def step_planes(state, lead, trail, j_halo, k_halo, winds, first, length, base):
    planes, full, k_size, heights = winds[0].shape
    rows = rows_for(first, length)
    steps = length // rows
    tail = (k_size, heights)
    halo = j_halo is not None
    top = planes - 1

    def plane_of(p):
        return p * top if halo else p + 1

    def block(offset, which):
        return pl.BlockSpec((1, rows) + tail, lambda p, g: (which(p), offset // rows + g, 0, 0))

    def one_row(row_of):
        return pl.BlockSpec((1, 1) + tail, lambda p, g: (plane_of(p), row_of(g), 0, 0))

    def low_of(p):
        return jnp.where(p == 0, 0, top - 1) if halo else p

    def high_of(p):
        return jnp.where(p == 0, 1, top) if halo else p + 2

    line = pl.BlockSpec((1, length, heights), lambda p, g: (plane_of(p), 0, 0))
    in_specs = [
        block(0, plane_of),
        one_row(lambda g: jnp.maximum(g * rows - 1, 0)),
        one_row(lambda g: jnp.minimum(g * rows + rows, length - 1)),
        one_row(lambda g: lead[1]),
        one_row(lambda g: trail[1]),
        block(0, low_of), block(0, high_of), line, line,
    ] + [block(first, plane_of)] * 3
    operands = [state, state, state, lead[0], trail[0], state, state, *k_halo, *winds]
    if halo:
        operands += j_halo
        in_specs += [
            pl.BlockSpec((rows,) + tail, lambda p, g: (jnp.where(p == 0, g, steps - 1), 0, 0)),
            pl.BlockSpec((rows,) + tail, lambda p, g: (jnp.where(p == 0, 0, g), 0, 0)),
        ]
    aliases = {}
    if base is not None:
        aliases = {len(operands): 0}
        operands.append(base)
        in_specs.append(pl.BlockSpec(memory_space=pl.ANY))
    count = 2 if halo else planes - 2
    cells = count * length * k_size * heights
    return pl.pallas_call(
        functools.partial(plane_kernel, rows=rows, halo=halo),
        grid=(count, steps),
        in_specs=in_specs,
        out_specs=block(first, plane_of),
        out_shape=jax.ShapeDtypeStruct((planes, full) + tail, state.dtype),
        input_output_aliases=aliases,
        cost_estimate=pl.CostEstimate(flops=25 * cells, bytes_accessed=24 * cells, transcendentals=0),
        compiler_params=pltpu.CompilerParams(dimension_semantics=("arbitrary", "arbitrary")),
    )(*operands)


def step_chunk(state, start, lead, trail, j_halo, k_halo, winds, first, length, edges, base):
    planes, full, k_size, heights = winds[0].shape
    rows = rows_for(start, first, length)
    steps = length // rows
    tail = (k_size, heights)

    def block(offset):
        return pl.BlockSpec((planes, rows) + tail, lambda g: (0, offset // rows + g, 0, 0))

    def one_row(row_of):
        return pl.BlockSpec((planes, 1) + tail, lambda g: (0, row_of(g), 0, 0))

    plane = pl.BlockSpec((rows,) + tail, lambda g: (g, 0, 0))
    line = pl.BlockSpec((planes, length, heights), lambda g: (0, 0, 0))
    in_specs = [
        block(start),
        one_row(lambda g: start + jnp.maximum(g * rows - 1, 0)),
        one_row(lambda g: start + jnp.minimum(g * rows + rows, length - 1)),
        one_row(lambda g: lead[1]),
        one_row(lambda g: trail[1]),
        plane, plane, line, line,
    ] + [block(first)] * 3
    operands = [state, state, state, lead[0], trail[0], *j_halo, *k_halo, *winds]
    aliases = {}
    dtype = state.dtype
    if edges:
        out_specs = [block(0), plane, plane, line, line]
        out_shape = [
            jax.ShapeDtypeStruct((planes, length) + tail, dtype),
            *[jax.ShapeDtypeStruct((length,) + tail, dtype)] * 2,
            *[jax.ShapeDtypeStruct((planes, length, heights), dtype)] * 2,
        ]
    else:
        out_specs = [block(first)]
        out_shape = [jax.ShapeDtypeStruct((planes, full) + tail, dtype)]
        if base is not None:
            aliases = {len(operands): 0}
            operands.append(base)
            in_specs.append(pl.BlockSpec(memory_space=pl.ANY))
    cells = planes * length * k_size * heights
    return pl.pallas_call(
        functools.partial(
            step_kernel, planes=planes, rows=rows, edges=edges, aliased=len(aliases)
        ),
        grid=(steps,),
        in_specs=in_specs,
        out_specs=out_specs,
        out_shape=out_shape,
        input_output_aliases=aliases,
        cost_estimate=pl.CostEstimate(flops=25 * cells, bytes_accessed=24 * cells, transcendentals=0),
        compiler_params=pltpu.CompilerParams(dimension_semantics=("arbitrary",)),
    )(*operands)


def chunk_lengths(full):
    if full % sum(CHUNK_EIGHTHS):
        return [full]
    return [full // sum(CHUNK_EIGHTHS) * eighths for eighths in CHUNK_EIGHTHS]


def on_device(initial_scalar_state, *winds):
    return all_steps(initial_scalar_state, winds)


def all_steps(x, winds):
    planes, full = x.shape[:2]
    lengths = chunk_lengths(full)
    chunks = len(lengths)
    firsts = [sum(lengths[:c]) for c in range(chunks)]
    j_halos, later = [], x
    for c in range(chunks):
        part = slice(firsts[c], firsts[c] + lengths[c])
        edges, later = lax.optimization_barrier(((later[0, part], later[-1, part]), later))
        j_halos.append(exchange_south(*edges))
    i_halo = exchange(later[:, :1], later[:, -1:], "east")
    k_halos = []
    for first, size in zip(firsts, lengths):
        part = later[:, first:first + size]
        k_halos.append(exchange(part[:, :, 0], part[:, :, -1], "down"))
    states = list(zip([x] * chunks, firsts))
    for step in range(STEPS):
        final = step == STEPS - 1
        base = None
        made = []
        for c in range(chunks):
            state, start = states[c]
            lead = (states[c - 1][0], states[c - 1][1] + lengths[c - 1] - 1) if c else (i_halo[0], 0)
            trail = states[c + 1] if c < chunks - 1 else (i_halo[1], 0)
            if final and c == chunks - 1 and planes > 2 and start == 0:
                same = (winds, firsts[c], lengths[c])
                base = step_planes(state, lead, trail, None, k_halos[c], *same, base)
                return step_planes(state, lead, trail, j_halos[c], k_halos[c], *same, base)
            out = step_chunk(
                state, start, lead, trail, j_halos[c], k_halos[c], winds, firsts[c],
                lengths[c], not final, base,
            )
            if final:
                base = out[0]
                continue
            fresh, first_plane, last_plane, k_first, k_last = out
            made.append((fresh, 0))
            j_halos[c] = exchange_south(first_plane, last_plane)
            k_halos[c] = exchange(k_first, k_last, "down")
        if final:
            return base
        states = made
        i_halo = exchange(made[0][0][:, :1], made[-1][0][:, -1:], "east")


def solution(mesh):
    placed = P("south", "east", "down", None)
    return jax.shard_map(
        on_device,
        mesh=mesh,
        in_specs=(placed,) * 4,
        out_specs=placed,
        check_vma=False,
    )
```

```python
import functools

import jax
import jax.numpy as jnp
from jax import lax
from jax.experimental import pallas as pl
from jax.experimental.pallas import tpu as pltpu
from jax.sharding import PartitionSpec as P


STEPS = 4
CHUNK_EIGHTHS = (4, 3, 1)
SMOOTH_RATE = 0.05


def shift(values, axis, step):
    size = lax.axis_size(axis)
    return lax.ppermute(values, axis, [(i, (i + step) % size) for i in range(size)])


def exchange(first, last, axis):
    if lax.axis_size(axis) == 2:
        other = shift(jnp.stack([last, first]), axis, 1)
        return other[0], other[1]
    return shift(last, axis, 1), shift(first, axis, -1)


def send_south(plane, way):
    return shift(plane, "south", 1 if way == "up" else -1)


def exchange_south(first, last):
    return send_south(last, "up"), send_south(first, "down")


def step_kernel(*refs, planes, rows, edges, aliased):
    (state, above_row, below_row, lead_row, trail_row, j_before, j_after,
     k_before, k_after, wind_j, wind_i, wind_k) = refs[:12]
    outs = refs[12 + aliased:]
    out = outs[0]
    at = pl.program_id(0)
    is_first, is_last = at == 0, at == pl.num_programs(0) - 1
    levels = lax.broadcasted_iota(jnp.int32, state.shape[2:], 0)
    k_size = state.shape[2]
    at_bottom, at_top = levels == 0, levels == k_size - 1
    for j in range(planes):
        for r in range(rows):
            row = at * rows + r
            here = state[j, r]
            i_low = state[j, r - 1] if r else jnp.where(is_first, lead_row[j, 0], above_row[j, 0])
            i_high = (
                state[j, r + 1] if r < rows - 1
                else jnp.where(is_last, trail_row[j, 0], below_row[j, 0])
            )
            j_low = state[j - 1, r] if j else j_before[r]
            j_high = state[j + 1, r] if j < planes - 1 else j_after[r]
            k_low = jnp.where(at_bottom, k_before[j, pl.ds(row, 1), :], pltpu.roll(here, 1, 0))
            k_high = jnp.where(
                at_top, k_after[j, pl.ds(row, 1), :], pltpu.roll(here, k_size - 1, 0)
            )
            spread = j_low + j_high + i_low + i_high + k_low + k_high - 6.0 * here
            new = (
                here
                - wind_j[j, r] * (j_high - j_low)
                - wind_i[j, r] * (i_high - i_low)
                - wind_k[j, r] * (k_high - k_low)
                + SMOOTH_RATE * spread
            )
            out[j, r] = new
            if edges:
                first_plane, last_plane, k_first, k_last = outs[1:]
                k_first[j, pl.ds(row, 1), :] = new[:1]
                k_last[j, pl.ds(row, 1), :] = new[k_size - 1:]
                if j == 0:
                    first_plane[r] = new
                if j == planes - 1:
                    last_plane[r] = new


def plane_kernel(*refs, rows, halo):
    (state, above_row, below_row, lead_row, trail_row, low, beyond,
     k_before, k_after, wind_j, wind_i, wind_k) = refs[:12]
    out = refs[-1]
    at = pl.program_id(1)
    is_first, is_last = at == 0, at == pl.num_programs(1) - 1
    is_start = pl.program_id(0) == 0
    levels = lax.broadcasted_iota(jnp.int32, state.shape[2:], 0)
    k_size = state.shape[2]
    at_bottom, at_top = levels == 0, levels == k_size - 1
    for r in range(rows):
        row = at * rows + r
        here = state[0, r]
        i_low = state[0, r - 1] if r else jnp.where(is_first, lead_row[0, 0], above_row[0, 0])
        i_high = (
            state[0, r + 1] if r < rows - 1
            else jnp.where(is_last, trail_row[0, 0], below_row[0, 0])
        )
        j_low = low[0, r]
        if halo:
            inner, j_before, j_after = j_low, beyond, refs[12]
            j_low = jnp.where(is_start, j_before[r], inner)
            j_high = jnp.where(is_start, inner, j_after[r])
        else:
            j_high = beyond[0, r]
        k_low = jnp.where(at_bottom, k_before[0, pl.ds(row, 1), :], pltpu.roll(here, 1, 0))
        k_high = jnp.where(at_top, k_after[0, pl.ds(row, 1), :], pltpu.roll(here, k_size - 1, 0))
        spread = j_low + j_high + i_low + i_high + k_low + k_high - 6.0 * here
        out[0, r] = (
            here
            - wind_j[0, r] * (j_high - j_low)
            - wind_i[0, r] * (i_high - i_low)
            - wind_k[0, r] * (k_high - k_low)
            + SMOOTH_RATE * spread
        )


def rows_for(*sizes):
    return next(n for n in (4, 2, 1) if all(size % n == 0 for size in sizes))


def step_planes(state, lead, trail, j_halo, k_halo, winds, first, length, base):
    planes, full, k_size, heights = winds[0].shape
    halo = j_halo is not None
    rows = min(rows_for(first, length), 2 if halo else 4)
    steps = length // rows
    tail = (k_size, heights)
    top = planes - 1

    def plane_of(p):
        return p * top if halo else p + 1

    def block(offset, which):
        return pl.BlockSpec((1, rows) + tail, lambda p, g: (which(p), offset // rows + g, 0, 0))

    def one_row(row_of):
        return pl.BlockSpec((1, 1) + tail, lambda p, g: (plane_of(p), row_of(g), 0, 0))

    def low_of(p):
        return jnp.where(p == 0, 1, top - 1) if halo else p

    if halo:
        beyond, after = j_halo
        beyond_spec = pl.BlockSpec(
            (rows,) + tail, lambda p, g: (jnp.where(p == 0, g, steps - 1), 0, 0)
        )
    else:
        beyond, beyond_spec = state, block(0, lambda p: p + 2)

    line = pl.BlockSpec((1, length, heights), lambda p, g: (plane_of(p), 0, 0))
    in_specs = [
        block(0, plane_of),
        one_row(lambda g: jnp.maximum(g * rows - 1, 0)),
        one_row(lambda g: jnp.minimum(g * rows + rows, length - 1)),
        one_row(lambda g: lead[1]),
        one_row(lambda g: trail[1]),
        block(0, low_of), beyond_spec, line, line,
    ] + [block(first, plane_of)] * 3
    operands = [state, state, state, lead[0], trail[0], state, beyond, *k_halo, *winds]
    if halo:
        operands.append(after)
        in_specs.append(
            pl.BlockSpec((rows,) + tail, lambda p, g: (jnp.where(p == 0, 0, g), 0, 0))
        )
    aliases = {}
    if base is not None:
        aliases = {len(operands): 0}
        operands.append(base)
        in_specs.append(pl.BlockSpec(memory_space=pl.ANY))
    count = 2 if halo else planes - 2
    cells = count * length * k_size * heights
    return pl.pallas_call(
        functools.partial(plane_kernel, rows=rows, halo=halo),
        grid=(count, steps),
        in_specs=in_specs,
        out_specs=block(first, plane_of),
        out_shape=jax.ShapeDtypeStruct((planes, full) + tail, state.dtype),
        input_output_aliases=aliases,
        cost_estimate=pl.CostEstimate(flops=25 * cells, bytes_accessed=24 * cells, transcendentals=0),
        compiler_params=pltpu.CompilerParams(dimension_semantics=("arbitrary", "arbitrary")),
    )(*operands)


def step_chunk(state, start, lead, trail, j_halo, k_halo, winds, first, length, edges, base):
    planes, full, k_size, heights = winds[0].shape
    rows = rows_for(start, first, length)
    steps = length // rows
    tail = (k_size, heights)

    def block(offset):
        return pl.BlockSpec((planes, rows) + tail, lambda g: (0, offset // rows + g, 0, 0))

    def one_row(row_of):
        return pl.BlockSpec((planes, 1) + tail, lambda g: (0, row_of(g), 0, 0))

    plane = pl.BlockSpec((rows,) + tail, lambda g: (g, 0, 0))
    line = pl.BlockSpec((planes, length, heights), lambda g: (0, 0, 0))
    in_specs = [
        block(start),
        one_row(lambda g: start + jnp.maximum(g * rows - 1, 0)),
        one_row(lambda g: start + jnp.minimum(g * rows + rows, length - 1)),
        one_row(lambda g: lead[1]),
        one_row(lambda g: trail[1]),
        plane, plane, line, line,
    ] + [block(first)] * 3
    operands = [state, state, state, lead[0], trail[0], *j_halo, *k_halo, *winds]
    aliases = {}
    dtype = state.dtype
    if edges:
        out_specs = [block(0), plane, plane, line, line]
        out_shape = [
            jax.ShapeDtypeStruct((planes, length) + tail, dtype),
            *[jax.ShapeDtypeStruct((length,) + tail, dtype)] * 2,
            *[jax.ShapeDtypeStruct((planes, length, heights), dtype)] * 2,
        ]
    else:
        out_specs = [block(first)]
        out_shape = [jax.ShapeDtypeStruct((planes, full) + tail, dtype)]
        if base is not None:
            aliases = {len(operands): 0}
            operands.append(base)
            in_specs.append(pl.BlockSpec(memory_space=pl.ANY))
    cells = planes * length * k_size * heights
    return pl.pallas_call(
        functools.partial(
            step_kernel, planes=planes, rows=rows, edges=edges, aliased=len(aliases)
        ),
        grid=(steps,),
        in_specs=in_specs,
        out_specs=out_specs,
        out_shape=out_shape,
        input_output_aliases=aliases,
        cost_estimate=pl.CostEstimate(flops=25 * cells, bytes_accessed=24 * cells, transcendentals=0),
        compiler_params=pltpu.CompilerParams(dimension_semantics=("arbitrary",)),
    )(*operands)


def chunk_lengths(full):
    if full % sum(CHUNK_EIGHTHS):
        return [full]
    return [full // sum(CHUNK_EIGHTHS) * eighths for eighths in CHUNK_EIGHTHS]


def on_device(initial_scalar_state, *winds):
    return all_steps(initial_scalar_state, winds)


def all_steps(x, winds):
    planes, full = x.shape[:2]
    lengths = chunk_lengths(full)
    chunks = len(lengths)
    firsts = [sum(lengths[:c]) for c in range(chunks)]
    j_halos, later = [], x
    for c in range(chunks):
        part = slice(firsts[c], firsts[c] + lengths[c])
        last, later = lax.optimization_barrier((later[-1, part], later))
        first, later = lax.optimization_barrier((later[0, part], later))
        j_halos.append(exchange_south(first, last))
    i_halo = exchange(later[:, :1], later[:, -1:], "east")
    k_halos = []
    for first, size in zip(firsts, lengths):
        part = later[:, first:first + size]
        k_halos.append(exchange(part[:, :, 0], part[:, :, -1], "down"))
    states = list(zip([x] * chunks, firsts))
    for step in range(STEPS):
        final = step == STEPS - 1
        base = None
        made = []

        def sides(c):
            before, after = c - 1, c + 1
            lead = (states[before][0], states[before][1] + lengths[before] - 1) if c else (i_halo[0], 0)
            return lead, states[after] if after < chunks else (i_halo[1], 0)

        split = final and chunks > 1 and planes > 2 and states[-1][1] == 0
        if split:
            same = (winds, firsts[-1], lengths[-1])
            base = step_planes(states[-1][0], *sides(chunks - 1), None, k_halos[-1], *same, base)
        for c in range(chunks):
            state, start = states[c]
            lead, trail = sides(c)
            if split and c == chunks - 1:
                return step_planes(state, lead, trail, j_halos[c], k_halos[c], *same, base)
            out = step_chunk(
                state, start, lead, trail, j_halos[c], k_halos[c], winds, firsts[c],
                lengths[c], not final, base,
            )
            if final:
                base = out[0]
                continue
            fresh, first_plane, last_plane, k_first, k_last = out
            made.append((fresh, 0))
            j_halos[c] = exchange_south(first_plane, last_plane)
            k_halos[c] = exchange(k_first, k_last, "down")
        if final:
            return base
        states = made
        i_halo = exchange(made[0][0][:, :1], made[-1][0][:, -1:], "east")


def solution(mesh):
    placed = P("south", "east", "down", None)
    return jax.shard_map(
        on_device,
        mesh=mesh,
        in_specs=(placed,) * 4,
        out_specs=placed,
        check_vma=False,
    )
```
